32 devices in a mesh: groups: 2 (over y), pair: 4 (over z), vir: 2 (over x), sub: 2 (over core).
Axes of the slice: x: 2, y: 2, z: 4, core: 2. Of those that a mesh axis runs over, the one named last changes fastest.
Arguments:
- amplitudes: bfloat16 [8, 36, 128, 128], P(('groups', 'pair'), 'vir', 'sub'), parts along dimension 0, may hold values from -1 to 1
- pair_list: int32 [8, 2], P(('groups', 'pair')), parts along dimension 0, may hold values from 0 to 255, as said below
- tile_list: int32 [36, 2], replicated, may hold values from 0 to 7, as said below
Outputs:
- p_virt: float32 [72, 128, 128], P(('groups', 'vir'), 'sub'), parts along dimension 0
- p_occ: float32 [512, 256], P('groups'), parts along dimension 0
The draws below stay inside these ranges and needn't reach their ends.
There are 2 independent parts, one for each index of `groups`. The reference program is written for one: setup_inputs(seed, part) draws one part's arguments, and reference() takes and returns one part's arrays. A program takes and returns all parts, laid end to end along the dimension named above; an argument that names none is the same for every part. Nothing has to cross between parts.
Inputs may be any that keep to these rules, and one draw needn't show every extreme that they name: `pair_list`: each row holds two different occupied orbitals in increasing order; no two rows are equal. `tile_list`: each row holds a tile row and a tile column, row <= column; every such couple of the 8 x 8 tile grid appears exactly once.
All inputs are finite; a program needn't handle non-finite values.
Results may differ from the reference program's by a relative error of at most 0.0003.
Values may be sent and summed in bfloat16 or wider, within the bound.
A program may use at most 64 MiB of HBM per device.

```python
import math
import jax
import jax.numpy as jnp
import numpy as np
from jax import lax

V = 1024
OCC = 256
TILE = 128
NTV = 8
NT = 36
NP = 4


mode_count = 4


def pair_table(key):
    window_width = min(OCC, NP // 4 + 16)
    first_np, second_np = np.triu_indices(window_width, 1)
    chosen = jax.random.permutation(jax.random.fold_in(key, 3), first_np.shape[0])[:NP]
    orbitals = jax.random.permutation(jax.random.fold_in(key, 5), OCC)[:window_width]
    first_name = orbitals[jnp.asarray(first_np, jnp.int32)[chosen]]
    second_name = orbitals[jnp.asarray(second_np, jnp.int32)[chosen]]
    return jnp.stack([jnp.minimum(first_name, second_name), jnp.maximum(first_name, second_name)], axis=1).astype(jnp.int32)


def draw_pair_list(key, part):
    return pair_table(jax.random.fold_in(key, 11))


def draw_tile_list(key, part):
    rows_np, cols_np = np.triu_indices(NTV)
    shuffled = jax.random.permutation(jax.random.fold_in(key, 7), NT)
    tile_rows = jnp.asarray(rows_np, jnp.int32)[shuffled]
    tile_cols = jnp.asarray(cols_np, jnp.int32)[shuffled]
    return jnp.stack([tile_rows, tile_cols], axis=1).astype(jnp.int32)


def draw_amplitudes(key, part):
    pair_rows = pair_table(jax.random.fold_in(key, 11))
    mixing = jax.random.normal(jax.random.fold_in(key, 13), (OCC, mode_count), jnp.float32)
    shapes_common = jax.random.normal(jax.random.fold_in(key, 17), (mode_count, NT, TILE, TILE), jnp.float32)
    own_part = jnp.clip(jax.random.normal(jax.random.fold_in(key, 19), (NP, NT, TILE, TILE), jnp.float32), -6.0, 6.0)
    shared_weight = 0.2
    mixture = mixing[pair_rows[:, 0]] + mixing[pair_rows[:, 1]]
    shared_part = jnp.einsum('pm,mstu->pstu', mixture, shapes_common)
    overall = 1.0 / math.sqrt(2.6 * V * math.sqrt(NP * V))
    return jnp.clip(overall * (own_part + shared_weight * shared_part), -1.0, 1.0).astype(jnp.bfloat16)


def setup_inputs(seed: int = 0, part: int = 0) -> dict:
    arg_keys = jax.random.split(jax.random.key(seed), 4)
    part_keys = jax.random.split(jax.random.fold_in(arg_keys[3], part), 4)
    amplitudes = draw_amplitudes(jax.random.fold_in(jax.random.fold_in(arg_keys[3], part), 71), part)
    pair_list = draw_pair_list(jax.random.fold_in(jax.random.fold_in(arg_keys[3], part), 71), part)
    tile_list = draw_tile_list(jax.random.fold_in(arg_keys[3], 71), part)
    return {"amplitudes": amplitudes, "pair_list": pair_list, "tile_list": tile_list}


def slot_table(tile_list):
    tile_grid = jnp.arange(NTV, dtype=jnp.int32)
    upper_hit = (tile_list[:, 0][None, None, :] == tile_grid[:, None, None]) & (tile_list[:, 1][None, None, :] == tile_grid[None, :, None])
    either_hit = upper_hit | jnp.transpose(upper_hit, (1, 0, 2))
    slot_ids = jnp.arange(NT, dtype=jnp.int32)
    return jnp.sum(jnp.where(either_hit, slot_ids[None, None, :], 0), axis=2).astype(jnp.int32)


def keep_upper(tile_list):
    on_diagonal = tile_list[:, 0] == tile_list[:, 1]
    in_tile = jnp.arange(TILE, dtype=jnp.int32)
    lower_part = in_tile[None, :] <= in_tile[:, None]
    return jnp.logical_not(on_diagonal[:, None, None] & lower_part[None])


def unpack(packed, slot_grid):
    gathered = packed[slot_grid]
    turned = jnp.swapaxes(gathered, 2, 3)
    tile_grid = jnp.arange(NTV, dtype=jnp.int32)
    on_or_above = (tile_grid[:, None] <= tile_grid[None, :])[:, :, None, None]
    on_or_below = (tile_grid[:, None] >= tile_grid[None, :])[:, :, None, None]
    nothing = jnp.zeros_like(gathered)
    whole = jnp.where(on_or_above, gathered, nothing) - jnp.where(on_or_below, turned, nothing)
    return jnp.transpose(whole, (0, 2, 1, 3)).reshape(V, V)


def occurrences(pair_rows):
    orbital = jnp.concatenate([pair_rows[:, 0], pair_rows[:, 1]])
    partner = jnp.concatenate([pair_rows[:, 1], pair_rows[:, 0]])
    pair_count = pair_rows.shape[0]
    parity = jnp.concatenate([jnp.ones((pair_count,), jnp.float32), -jnp.ones((pair_count,), jnp.float32)])
    return orbital, partner, parity


def occ_density(pair_gram, left_pairs, right_pairs):
    left_orb, left_partner, left_sign = occurrences(left_pairs)
    right_orb, right_partner, right_sign = occurrences(right_pairs)
    doubled = jnp.tile(pair_gram, (2, 2))
    couple = jnp.where(left_partner[:, None] == right_partner[None, :], left_sign[:, None] * right_sign[None, :] * doubled, 0.0)
    orbitals = jnp.arange(OCC, dtype=jnp.int32)
    left_hot = (left_orb[:, None] == orbitals[None, :]).astype(jnp.float32)
    right_hot = (right_orb[:, None] == orbitals[None, :]).astype(jnp.float32)
    inner_sum = jnp.dot(couple, right_hot, precision=lax.Precision.HIGHEST)
    return -jnp.dot(left_hot.T, inner_sum, precision=lax.Precision.HIGHEST)


def reference(amplitudes, pair_list, tile_list):
    keep_mask = keep_upper(tile_list)
    masked = jnp.where(keep_mask[None], amplitudes, jnp.zeros((), jnp.bfloat16))
    slot_grid = slot_table(tile_list)

    def add_pair(running, packed):
        whole = unpack(packed, slot_grid)
        return running + jnp.dot(whole, whole.T, preferred_element_type=jnp.float32), None

    density, _ = lax.scan(add_pair, jnp.zeros((V, V), jnp.float32), masked)
    tile_view = jnp.transpose(density.reshape(NTV, TILE, NTV, TILE), (0, 2, 1, 3))
    p_virt = tile_view[tile_list[:, 0], tile_list[:, 1]]
    flat_masked = masked.reshape(NP, NT * TILE * TILE)
    flat_all = amplitudes.reshape(NP, NT * TILE * TILE)
    pair_gram = lax.dot_general(flat_masked, flat_all, (((1,), (1,)), ((), ())), preferred_element_type=jnp.float32)
    p_occ = occ_density(pair_gram, pair_list, pair_list)
    return (p_virt, p_occ)
```

```python
import functools
import math

import jax
import jax.numpy as jnp
from jax import lax
from jax.experimental import pallas as pl
from jax.experimental.pallas import tpu as pltpu
from jax.sharding import PartitionSpec as P

OCC = 256
GR = 16
LANES = 128
MESH = pl.DeviceIdType.MESH
F32 = jnp.float32
BF16 = jnp.bfloat16


def tile_table(tile_list, nt, ntv):
    grid = jnp.arange(ntv, dtype=jnp.int32)
    low = jnp.minimum(grid[:, None], grid[None, :])
    high = jnp.maximum(grid[:, None], grid[None, :])
    hit = (tile_list[:, 0][None, None] == low[:, :, None]) & (
        tile_list[:, 1][None, None] == high[:, :, None]
    )
    slots = jnp.arange(nt, dtype=jnp.int32)
    found = jnp.sum(jnp.where(hit, slots[None, None], 0), axis=2)
    return (found + jnp.where(grid[:, None] > grid[None, :], nt, 0)).reshape(-1)


def kernel(dims, amp, pairs, tiles, table, virt, occ, full, tile_buf, ga, acc, msg_s, msg_x,
           msg_z, part, landed, orb_buf, couple_buf,
           x_s, x_r, d_s, d_r, y_s, y_r, a_s, a_r, gs_s, gs_r, gx_s, gx_r, gz_s, gz_r,
           rs_s, rs_r, ag_s, ag_r):
    nz, nx, ns, pd, sd, gs, cg, nt, ntv, nch = dims
    n = nz * pd
    occs = 2 * n
    rd = gs * GR
    tw = ns * rd
    z_at = lax.axis_index("pair")
    x_at = lax.axis_index("vir")
    s_at = lax.axis_index("sub")
    sizes = {"pair": nz, "vir": nx, "sub": ns}
    here = {"pair": z_at, "vir": x_at, "sub": s_at}

    def ahead(axis, by):
        return lax.rem(here[axis] + by, sizes[axis])

    def behind(axis, by):
        return lax.rem(here[axis] + sizes[axis] - by, sizes[axis])

    def send(src, dst, s_sem, r_sem, axis, by):
        return pltpu.make_async_remote_copy(
            src_ref=src, dst_ref=dst, send_sem=s_sem, recv_sem=r_sem,
            device_id={axis: ahead(axis, by)}, device_id_type=MESH)

    barrier = pltpu.get_barrier_semaphore()
    count = 0
    for axis in ("sub", "vir", "pair"):
        for by in range(1, sizes[axis]):
            pl.semaphore_signal(barrier, inc=1, device_id={axis: ahead(axis, by)},
                                device_id_type=MESH)
            count += 1
    pl.semaphore_wait(barrier, count)

    step = sd // nch * gs

    def x_copy(by, ch):
        rows = pl.ds(ch * step, step)
        return send(amp.at[:, rows], full.at[x_at, s_at, :, rows], x_s.at[by - 1, ch],
                    x_r.at[by - 1, ch], "vir", by)

    def relay(by, hop, ch):
        rows = pl.ds(ch * step, step)
        at = full.at[behind("vir", by), s_at, :, rows]
        return send(at, at, y_s.at[hop - 1, by - 1, ch], y_r.at[hop - 1, by - 1, ch], "sub", hop)

    def own_copy(hop):
        return send(amp, full.at[x_at, s_at], d_s.at[hop - 1], d_r.at[hop - 1], "sub", hop)

    def a2a_copy(by):
        rows = pl.ds(ahead("pair", by) * cg, cg)
        return send(amp.at[:, rows], ga.at[z_at], a_s.at[by - 1], a_r.at[by - 1], "pair", by)

    for ch in range(nch):
        for by in range(1, nx):
            x_copy(by, ch).start()
    for hop in range(1, ns):
        own_copy(hop).start()
    for by in range(1, nz):
        a2a_copy(by).start()

    full[x_at, s_at] = amp[...]
    ga[z_at] = amp[:, pl.ds(z_at * cg, cg)]
    lane_of = lax.broadcasted_iota(jnp.int32, (tw, LANES), 1)
    row_of = lax.broadcasted_iota(jnp.int32, (tw, LANES), 0)
    lower = lane_of <= row_of

    def build(x_from, lo, hi):
        def one(local, carry):
            slot = x_from * sd + local
            diagonal = tiles[slot, 0] == tiles[slot, 1]
            dropped = lower & diagonal
            groups = pl.ds(local * gs, gs)
            for k in range(pd):
                whole = jnp.concatenate(
                    [full[x_from, s, k, groups].reshape(rd, LANES) for s in range(ns)], axis=0)
                kept = jnp.where(dropped, 0.0, whole.astype(F32))
                turned = kept.T
                tile_buf[k, slot] = (kept - jnp.where(diagonal, turned, 0.0)).astype(BF16)
                tile_buf[k, nt + slot] = (-turned).astype(BF16)
            return carry

        lax.fori_loop(lo, hi, one, 0)

    for hop in range(1, ns):
        own_copy(hop).wait_recv()
    build(x_at, 0, sd)

    for by in range(1, nz):
        a2a_copy(by).wait_recv()
    acc[...] = jnp.zeros_like(acc)
    g_lane = lax.broadcasted_iota(jnp.int32, (GR, LANES), 1)
    g_row = lax.broadcasted_iota(jnp.int32, (GR, LANES), 0)

    def gram_group(i, carry):
        at = z_at * cg + i
        slot = x_at * sd + jnp.minimum(at // gs, sd - 1)
        diagonal = tiles[slot, 0] == tiles[slot, 1]
        dropped = (g_lane <= g_row + (s_at * rd + lax.rem(at, gs) * GR)) & diagonal
        vals = ga[:, :, i].reshape(n, GR, LANES).astype(F32)
        vals = jnp.where(dropped[None], 0.0, vals)
        for p in range(n):
            acc[p] += vals * vals[p : p + 1]
        return carry

    lax.fori_loop(0, cg, gram_group, 0)
    m_lane = lax.broadcasted_iota(jnp.int32, (n, LANES), 1)
    grid = jnp.zeros((n, LANES), F32)
    for p in range(n):
        col = jnp.sum(jnp.sum(acc[p], axis=1), axis=1, keepdims=True)
        grid = jnp.where((m_lane == p) | (m_lane == p + n), col, grid)
    msg_s[0, 0:n] = grid
    msg_s[0, n:occs] = grid

    def gs_copy(hop):
        return send(msg_s.at[0], msg_s.at[hop], gs_s.at[hop - 1], gs_r.at[hop - 1], "sub", hop)

    def gx_copy(by):
        return send(msg_x.at[0], msg_x.at[by], gx_s.at[by - 1], gx_r.at[by - 1], "vir", by)

    def gz_copy(by):
        return send(msg_z.at[z_at], msg_z.at[z_at], gz_s.at[by - 1], gz_r.at[by - 1], "pair", by)

    for hop in range(1, ns):
        gs_copy(hop).start()

    for by in range(1, nx):
        for ch in range(nch):
            x_copy(by, ch).wait_recv()
            for hop in range(1, ns):
                relay(by, hop, ch).start()
            if ch == 0 and by == 1:
                total = msg_s[0]
                for hop in range(1, ns):
                    gs_copy(hop).wait_recv()
                    total = total + msg_s[hop]
                msg_x[0] = total
                for other in range(1, nx):
                    gx_copy(other).start()
            for hop in range(1, ns):
                relay(by, hop, ch).wait_recv()
            build(behind("vir", by), ch * (sd // nch), (ch + 1) * (sd // nch))

    total = msg_x[0]
    for by in range(1, nx):
        gx_copy(by).wait_recv()
        total = total + msg_x[by]
    msg_z[z_at, 0:occs] = total
    for k in range(pd):
        for e in range(2):
            msg_z[z_at, pl.ds(occs + 2 * k + e, 1)] = jnp.full((1, LANES), pairs[k, e], jnp.int32).astype(F32)
    for by in range(1, nz):
        gz_copy(by).start()

    if part.shape[0] > sd * gs:
        part[pl.ds(sd * gs, part.shape[0] - sd * gs)] = jnp.zeros(
            (part.shape[0] - sd * gs, GR, LANES), F32)

    def virt_slot(local, carry):
        slot = x_at * sd + local
        r = tiles[slot, 0]
        c = tiles[slot, 1]
        rows = pl.ds(pl.multiple_of(s_at * rd, rd), rd)
        total = None
        for k in range(pd):
            left = jnp.concatenate(
                [tile_buf[k, table[r * ntv + j], rows] for j in range(ntv)], axis=1)
            right = jnp.concatenate(
                [tile_buf[k, table[j * ntv + c]] for j in range(ntv)], axis=0)
            term = jnp.dot(left, right, preferred_element_type=F32)
            total = term if total is None else total + term
        part[pl.ds(local * gs, gs)] = (-total).reshape(gs, GR, LANES)
        return carry

    lax.fori_loop(0, sd, virt_slot, 0)

    def rs_copy(by):
        rows = pl.ds(ahead("pair", by) * cg, cg)
        return send(part.at[rows], landed.at[by - 1], rs_s.at[by - 1], rs_r.at[by - 1], "pair", by)

    own = pl.ds(z_at * cg, cg)

    def ag_copy(by):
        return send(virt.at[own], virt.at[own], ag_s.at[by - 1], ag_r.at[by - 1], "pair", by)

    for by in range(1, nz):
        rs_copy(by).start()

    for by in range(1, nz):
        gz_copy(by).wait_recv()
    gram = msg_z[0, 0:occs]
    for z in range(1, nz):
        gram = gram + msg_z[z, 0:occs]
    o_lane = lax.broadcasted_iota(jnp.int32, (1, LANES), 1)
    orb_lane = jnp.full((1, LANES), -1.0, F32)
    par_lane = jnp.full((1, LANES), -1.0, F32)
    orb_buf[...] = jnp.full(orb_buf.shape, -1.0, F32)
    for u in range(occs):
        p, e = u % n, u // n
        base = occs + 2 * (p % pd)
        orb = msg_z[p // pd, base + e : base + e + 1]
        par = msg_z[p // pd, base + 1 - e : base + 2 - e]
        orb_lane = jnp.where(o_lane == u, orb, orb_lane)
        par_lane = jnp.where(o_lane == u, par, par_lane)
        orb_buf[0, u : u + 1] = orb
        orb_buf[1, u : u + 1] = par
    c_lane = lax.broadcasted_iota(jnp.int32, (occs, LANES), 1)
    c_row = lax.broadcasted_iota(jnp.int32, (occs, LANES), 0)
    signed = jnp.where((c_lane < n) == (c_row < n), -gram, gram)
    couple_buf[...] = jnp.zeros_like(couple_buf)
    couple_buf[0:occs] = jnp.where(orb_buf[1, 0:occs] == par_lane, signed, 0.0)
    right_hot = (jnp.concatenate([orb_buf[0]] * (OCC // LANES), axis=1)
                 == lax.broadcasted_iota(jnp.int32, (LANES, OCC), 1).astype(F32)).astype(F32)
    left_hot = (lax.broadcasted_iota(jnp.int32, (OCC, LANES), 0).astype(F32)
                == orb_lane).astype(F32)
    inner = jnp.dot(couple_buf[...], right_hot, precision=lax.Precision.HIGHEST,
                    preferred_element_type=F32)
    occ[...] = jnp.dot(left_hot, inner, precision=lax.Precision.HIGHEST,
                       preferred_element_type=F32)

    for by in range(1, nz):
        rs_copy(by).wait_recv()
    total = part[own]
    for by in range(1, nz):
        total = total + landed[by - 1]
    virt[own] = total
    for by in range(1, nz):
        ag_copy(by).start()
    for by in range(1, nz):
        ag_copy(by).wait_recv()

    for by in range(1, nx):
        gx_copy(by).wait_send()
        for ch in range(nch):
            x_copy(by, ch).wait_send()
            for hop in range(1, ns):
                relay(by, hop, ch).wait_send()
    for hop in range(1, ns):
        own_copy(hop).wait_send()
        gs_copy(hop).wait_send()
    for by in range(1, nz):
        a2a_copy(by).wait_send()
        gz_copy(by).wait_send()
        rs_copy(by).wait_send()
        ag_copy(by).wait_send()


def shards(sizes, amplitudes, pair_list, tile_list):
    nz, nx, ns = sizes
    pd, sd, rd, _ = amplitudes.shape
    nt = tile_list.shape[0]
    ntv = (math.isqrt(8 * nt + 1) - 1) // 2
    gs = rd // GR
    ng = sd * gs
    cg = -(-ng // nz)
    ngp = cg * nz
    nch = 3 if sd % 3 == 0 else 1
    n = nz * pd
    occs = 2 * n
    amp = amplitudes.reshape(pd, ng, GR, LANES)
    if ngp > ng:
        amp = jnp.pad(amp, ((0, 0), (0, ngp - ng), (0, 0), (0, 0)))
    mr = -(-(occs + 2 * pd) // 8) * 8
    dims = (nz, nx, ns, pd, sd, gs, cg, nt, ntv, nch)
    vmem = pl.BlockSpec(memory_space=pltpu.VMEM)
    smem = pl.BlockSpec(memory_space=pltpu.SMEM)

    def dma(*shape):
        return pltpu.SemaphoreType.DMA(tuple(max(1, d) for d in shape))

    sems = []
    for shape in ((nx - 1, nch), (ns - 1,), (ns - 1, nx - 1, nch), (nz - 1,), (ns - 1,),
                  (nx - 1,), (nz - 1,), (nz - 1,), (nz - 1,)):
        sems += [dma(*shape), dma(*shape)]
    virt, occ = pl.pallas_call(
        functools.partial(kernel, dims),
        out_shape=(jax.ShapeDtypeStruct((ngp, GR, LANES), F32),
                   jax.ShapeDtypeStruct((OCC, OCC), F32)),
        in_specs=[vmem, smem, smem, smem],
        out_specs=(vmem, vmem),
        scratch_shapes=[
            pltpu.VMEM((nx, ns, pd, ngp, GR, LANES), BF16),
            pltpu.VMEM((pd, 2 * nt, ns * rd, LANES), BF16),
            pltpu.VMEM((nz, pd, cg, GR, LANES), BF16),
            pltpu.VMEM((n, n, GR, LANES), F32),
            pltpu.VMEM((ns, occs, LANES), F32),
            pltpu.VMEM((nx, occs, LANES), F32),
            pltpu.VMEM((nz, mr, LANES), F32),
            pltpu.VMEM((ngp, GR, LANES), F32),
            pltpu.VMEM((max(1, nz - 1), cg, GR, LANES), F32),
            pltpu.VMEM((2, LANES, LANES), F32),
            pltpu.VMEM((LANES, LANES), F32),
            *sems,
        ],
        compiler_params=pltpu.CompilerParams(
            collective_id=0, has_side_effects=True, vmem_limit_bytes=48 * 1024 * 1024),
    )(amp, pair_list, tile_list, tile_table(tile_list, nt, ntv))
    return (virt[:ng].reshape(sd, rd, LANES), occ)


def solution(mesh):
    in_specs = (P(("groups", "pair"), "vir", "sub", None), P(("groups", "pair"), None), P())
    out_specs = (P(("groups", "vir"), "sub", None), P("groups", None))
    sizes = (mesh.shape["pair"], mesh.shape["vir"], mesh.shape["sub"])
    return jax.shard_map(functools.partial(shards, sizes), mesh=mesh, in_specs=in_specs,
                         out_specs=out_specs, check_vma=False)
```

```python
import functools
import math

import jax
import jax.numpy as jnp
from jax import lax
from jax.experimental import pallas as pl
from jax.experimental.pallas import tpu as pltpu
from jax.sharding import PartitionSpec as P

OCC = 256
GR = 16
LANES = 128
LEVELS = 32767.0
MESH = pl.DeviceIdType.MESH
F32 = jnp.float32
BF16 = jnp.bfloat16


def tile_table(tile_list, nt, ntv):
    grid = jnp.arange(ntv, dtype=jnp.int32)
    low = jnp.minimum(grid[:, None], grid[None, :])
    high = jnp.maximum(grid[:, None], grid[None, :])
    hit = (tile_list[:, 0][None, None] == low[:, :, None]) & (
        tile_list[:, 1][None, None] == high[:, :, None]
    )
    slots = jnp.arange(nt, dtype=jnp.int32)
    found = jnp.sum(jnp.where(hit, slots[None, None], 0), axis=2)
    return (found + jnp.where(grid[:, None] > grid[None, :], nt, 0)).reshape(-1)


def squeeze(vals):
    peak = jnp.maximum(jnp.max(jnp.abs(vals), axis=1, keepdims=True), 1e-33)
    whole = jnp.round(vals * (LEVELS / peak)).astype(jnp.int32)
    return whole.astype(jnp.int16), peak * (1.0 / LEVELS)


def widen(whole, scale):
    return whole.astype(jnp.int32).astype(F32) * scale


def kernel(dims, amp_in, pairs, tiles, table, fin, fin_scale, occ, amp, full, tile_buf, ga, acc,
           msg_s, msg_x, msg_z, part, part_q, part_scale, landed, landed_scale, orb_buf,
           couple_buf, in_sem, x_s, x_r, d_s, d_r, y_s, y_r, a_s, a_r, gs_s, gs_r, gx_s, gx_r, gz_s, gz_r,
           rs_s, rs_r, ag_s, ag_r, rt_s, rt_r, at_s, at_r):
    nz, nx, ns, pd, sd, gs, cg, nt, ntv, nch = dims
    n = nz * pd
    occs = 2 * n
    rd = gs * GR
    tw = ns * rd
    z_at = lax.axis_index("pair")
    x_at = lax.axis_index("vir")
    s_at = lax.axis_index("sub")
    sizes = {"pair": nz, "vir": nx, "sub": ns}
    here = {"pair": z_at, "vir": x_at, "sub": s_at}

    def ahead(axis, by):
        return lax.rem(here[axis] + by, sizes[axis])

    def behind(axis, by):
        return lax.rem(here[axis] + sizes[axis] - by, sizes[axis])

    def send(src, dst, s_sem, r_sem, axis, by):
        return pltpu.make_async_remote_copy(
            src_ref=src, dst_ref=dst, send_sem=s_sem, recv_sem=r_sem,
            device_id={axis: ahead(axis, by)}, device_id_type=MESH)

    fetch = pltpu.make_async_copy(amp_in, amp, in_sem)
    fetch.start()
    barrier = pltpu.get_barrier_semaphore()
    count = 0
    for axis in ("sub", "vir", "pair"):
        for by in range(1, sizes[axis]):
            pl.semaphore_signal(barrier, inc=1, device_id={axis: ahead(axis, by)},
                                device_id_type=MESH)
            count += 1
    pl.semaphore_wait(barrier, count)
    fetch.wait()

    step = sd // nch * gs

    def x_copy(by, ch):
        rows = pl.ds(ch * step, step)
        return send(amp.at[:, rows], full.at[x_at, s_at, :, rows], x_s.at[by - 1, ch],
                    x_r.at[by - 1, ch], "vir", by)

    def relay(by, hop, ch):
        rows = pl.ds(ch * step, step)
        at = full.at[behind("vir", by), s_at, :, rows]
        return send(at, at, y_s.at[hop - 1, by - 1, ch], y_r.at[hop - 1, by - 1, ch], "sub", hop)

    def own_copy(hop):
        return send(amp, full.at[x_at, s_at], d_s.at[hop - 1], d_r.at[hop - 1], "sub", hop)

    def a2a_copy(by):
        rows = pl.ds(ahead("pair", by) * cg, cg)
        return send(amp.at[:, rows], ga.at[z_at], a_s.at[by - 1], a_r.at[by - 1], "pair", by)

    for ch in range(nch):
        for by in range(1, nx):
            x_copy(by, ch).start()
    for hop in range(1, ns):
        own_copy(hop).start()
    for by in range(1, nz):
        a2a_copy(by).start()

    full[x_at, s_at] = amp[...]
    ga[z_at] = amp[:, pl.ds(z_at * cg, cg)]
    lane_of = lax.broadcasted_iota(jnp.int32, (tw, LANES), 1)
    row_of = lax.broadcasted_iota(jnp.int32, (tw, LANES), 0)
    lower = lane_of <= row_of

    def build(x_from, lo, hi):
        def one(local, carry):
            slot = x_from * sd + local
            diagonal = tiles[slot, 0] == tiles[slot, 1]
            dropped = lower & diagonal
            groups = pl.ds(local * gs, gs)
            for k in range(pd):
                whole = jnp.concatenate(
                    [full[x_from, s, k, groups].reshape(rd, LANES) for s in range(ns)], axis=0)
                kept = jnp.where(dropped, 0.0, whole.astype(F32))
                turned = kept.T
                tile_buf[k, slot] = (kept - jnp.where(diagonal, turned, 0.0)).astype(BF16)
                tile_buf[k, nt + slot] = (-turned).astype(BF16)
            return carry

        lax.fori_loop(lo, hi, one, 0)

    for hop in range(1, ns):
        own_copy(hop).wait_recv()
    build(x_at, 0, sd)

    for by in range(1, nx):
        for ch in range(nch):
            x_copy(by, ch).wait_recv()
            for hop in range(1, ns):
                relay(by, hop, ch).start()
            for hop in range(1, ns):
                relay(by, hop, ch).wait_recv()
            build(behind("vir", by), ch * (sd // nch), (ch + 1) * (sd // nch))

    if part.shape[0] > sd * gs:
        spare = pl.ds(sd * gs, part.shape[0] - sd * gs)
        part[spare] = jnp.zeros((part.shape[0] - sd * gs, GR, LANES), F32)
        part_q[spare] = jnp.zeros((part.shape[0] - sd * gs, GR, LANES), jnp.int16)
        part_scale[spare] = jnp.zeros((part.shape[0] - sd * gs, 1, LANES), F32)

    def virt_slot(local, carry):
        slot = x_at * sd + local
        r = tiles[slot, 0]
        c = tiles[slot, 1]
        rows = pl.ds(pl.multiple_of(s_at * rd, rd), rd)
        total = None
        for k in range(pd):
            left = jnp.concatenate(
                [tile_buf[k, table[r * ntv + j], rows] for j in range(ntv)], axis=1)
            right = jnp.concatenate(
                [tile_buf[k, table[j * ntv + c]] for j in range(ntv)], axis=0)
            term = jnp.dot(left, right, preferred_element_type=F32)
            total = term if total is None else total + term
        groups = pl.ds(local * gs, gs)
        total = (-total).reshape(gs, GR, LANES)
        part[groups] = total
        part_q[groups], part_scale[groups] = squeeze(total)
        return carry

    def rs_copies(to, source):
        rows = pl.ds(to * cg, cg)
        return [
            pltpu.make_async_remote_copy(
                src_ref=src.at[rows], dst_ref=dst.at[source], send_sem=s_sem.at[to],
                recv_sem=r_sem.at[source], device_id={"pair": to}, device_id_type=MESH)
            for src, dst, s_sem, r_sem in ((part_q, landed, rs_s, rs_r),
                                           (part_scale, landed_scale, rt_s, rt_r))
        ]

    own = pl.ds(z_at * cg, cg)

    def ag_copies(by):
        return [
            send(ref.at[own], ref.at[own], s_sem.at[by - 1], r_sem.at[by - 1], "pair", by)
            for ref, s_sem, r_sem in ((fin, ag_s, ag_r), (fin_scale, at_s, at_r))
        ]

    done = 0
    for to in range(nz):
        until = min(sd, -(-cg * (to + 1) // gs))
        if until > done:
            lax.fori_loop(done, until, virt_slot, 0)
            done = until

        @pl.when(z_at != to)
        def _():
            for copy in rs_copies(to, z_at):
                copy.start()

    for by in range(1, nz):
        a2a_copy(by).wait_recv()
    acc[...] = jnp.zeros_like(acc)
    g_lane = lax.broadcasted_iota(jnp.int32, (GR, LANES), 1)
    g_row = lax.broadcasted_iota(jnp.int32, (GR, LANES), 0)

    def gram_group(i, carry):
        at = z_at * cg + i
        slot = x_at * sd + jnp.minimum(at // gs, sd - 1)
        diagonal = tiles[slot, 0] == tiles[slot, 1]
        dropped = (g_lane <= g_row + (s_at * rd + lax.rem(at, gs) * GR)) & diagonal
        vals = ga[:, :, i].reshape(n, GR, LANES).astype(F32)
        vals = jnp.where(dropped[None], 0.0, vals)
        for p in range(n):
            acc[p] += vals * vals[p : p + 1]
        return carry

    lax.fori_loop(0, cg, gram_group, 0)
    m_lane = lax.broadcasted_iota(jnp.int32, (n, LANES), 1)
    grid = jnp.zeros((n, LANES), F32)
    for p in range(n):
        col = jnp.sum(jnp.sum(acc[p], axis=1), axis=1, keepdims=True)
        grid = jnp.where((m_lane == p) | (m_lane == p + n), col, grid)
    msg_s[0, 0:n] = grid
    msg_s[0, n:occs] = grid

    def gs_copy(hop):
        return send(msg_s.at[0], msg_s.at[hop], gs_s.at[hop - 1], gs_r.at[hop - 1], "sub", hop)

    def gx_copy(by):
        return send(msg_x.at[0], msg_x.at[by], gx_s.at[by - 1], gx_r.at[by - 1], "vir", by)

    def gz_copy(by):
        return send(msg_z.at[z_at], msg_z.at[z_at], gz_s.at[by - 1], gz_r.at[by - 1], "pair", by)

    for hop in range(1, ns):
        gs_copy(hop).start()

    for hop in range(1, ns):
        gs_copy(hop).wait_recv()
    msg_x[0] = sum((msg_s[hop] for hop in range(1, ns)), msg_s[0])
    for by in range(1, nx):
        gx_copy(by).start()
    total = msg_x[0]
    for by in range(1, nx):
        gx_copy(by).wait_recv()
        total = total + msg_x[by]
    msg_z[z_at, 0:occs] = total
    for k in range(pd):
        for e in range(2):
            msg_z[z_at, pl.ds(occs + 2 * k + e, 1)] = jnp.full((1, LANES), pairs[k, e], jnp.int32).astype(F32)
    for by in range(1, nz):
        gz_copy(by).start()

    total = part[own]
    for by in range(1, nz):
        source = behind("pair", by)
        for copy in rs_copies(source, source):
            copy.wait_recv()
        total = total + widen(landed[source], landed_scale[source])
    fin[own], fin_scale[own] = squeeze(total)
    for by in range(1, nz):
        for copy in ag_copies(by):
            copy.start()

    for by in range(1, nz):
        gz_copy(by).wait_recv()
    gram = msg_z[0, 0:occs]
    for z in range(1, nz):
        gram = gram + msg_z[z, 0:occs]
    o_lane = lax.broadcasted_iota(jnp.int32, (1, LANES), 1)
    orb_lane = jnp.full((1, LANES), -1.0, F32)
    par_lane = jnp.full((1, LANES), -1.0, F32)
    orb_buf[...] = jnp.full(orb_buf.shape, -1.0, F32)
    for u in range(occs):
        p, e = u % n, u // n
        base = occs + 2 * (p % pd)
        orb = msg_z[p // pd, base + e : base + e + 1]
        par = msg_z[p // pd, base + 1 - e : base + 2 - e]
        orb_lane = jnp.where(o_lane == u, orb, orb_lane)
        par_lane = jnp.where(o_lane == u, par, par_lane)
        orb_buf[0, u : u + 1] = orb
        orb_buf[1, u : u + 1] = par
    c_lane = lax.broadcasted_iota(jnp.int32, (occs, LANES), 1)
    c_row = lax.broadcasted_iota(jnp.int32, (occs, LANES), 0)
    signed = jnp.where((c_lane < n) == (c_row < n), -gram, gram)
    couple_buf[...] = jnp.zeros_like(couple_buf)
    couple_buf[0:occs] = jnp.where(orb_buf[1, 0:occs] == par_lane, signed, 0.0)
    right_hot = (jnp.concatenate([orb_buf[0]] * (OCC // LANES), axis=1)
                 == lax.broadcasted_iota(jnp.int32, (LANES, OCC), 1).astype(F32)).astype(F32)
    left_hot = (lax.broadcasted_iota(jnp.int32, (OCC, LANES), 0).astype(F32)
                == orb_lane).astype(F32)
    inner = jnp.dot(couple_buf[...], right_hot, precision=lax.Precision.HIGHEST,
                    preferred_element_type=F32)
    occ[...] = jnp.dot(left_hot, inner, precision=lax.Precision.HIGHEST,
                       preferred_element_type=F32)

    for by in range(1, nz):
        for copy in ag_copies(by):
            copy.wait_recv()

    for by in range(1, nx):
        gx_copy(by).wait_send()
        for ch in range(nch):
            x_copy(by, ch).wait_send()
            for hop in range(1, ns):
                relay(by, hop, ch).wait_send()
    for hop in range(1, ns):
        own_copy(hop).wait_send()
        gs_copy(hop).wait_send()
    for by in range(1, nz):
        a2a_copy(by).wait_send()
        gz_copy(by).wait_send()
        for copy in ag_copies(by) + rs_copies(ahead("pair", by), z_at):
            copy.wait_send()


def shards(sizes, amplitudes, pair_list, tile_list):
    nz, nx, ns = sizes
    pd, sd, rd, _ = amplitudes.shape
    nt = tile_list.shape[0]
    ntv = (math.isqrt(8 * nt + 1) - 1) // 2
    gs = rd // GR
    ng = sd * gs
    cg = -(-ng // nz)
    ngp = cg * nz
    nch = 6 if sd % 6 == 0 else 3 if sd % 3 == 0 else 1
    n = nz * pd
    occs = 2 * n
    amp = amplitudes.reshape(pd, ng, GR, LANES)
    if ngp > ng:
        amp = jnp.pad(amp, ((0, 0), (0, ngp - ng), (0, 0), (0, 0)))
    mr = -(-(occs + 2 * pd) // 8) * 8
    dims = (nz, nx, ns, pd, sd, gs, cg, nt, ntv, nch)
    vmem = pl.BlockSpec(memory_space=pltpu.VMEM)
    smem = pl.BlockSpec(memory_space=pltpu.SMEM)

    def dma(*shape):
        return pltpu.SemaphoreType.DMA(tuple(max(1, d) for d in shape))

    sems = []
    for shape in ((nx - 1, nch), (ns - 1,), (ns - 1, nx - 1, nch), (nz - 1,), (ns - 1,),
                  (nx - 1,), (nz - 1,), (nz,), (nz - 1,), (nz,), (nz - 1,)):
        sems += [dma(*shape), dma(*shape)]
    fin, scale, occ = pl.pallas_call(
        functools.partial(kernel, dims),
        out_shape=(jax.ShapeDtypeStruct((ngp, GR, LANES), jnp.int16),
                   jax.ShapeDtypeStruct((ngp, 1, LANES), F32),
                   jax.ShapeDtypeStruct((OCC, OCC), F32)),
        in_specs=[pl.BlockSpec(memory_space=pl.ANY), smem, smem, smem],
        out_specs=(vmem, vmem, vmem),
        scratch_shapes=[
            pltpu.VMEM((pd, ngp, GR, LANES), BF16),
            pltpu.VMEM((nx, ns, pd, ngp, GR, LANES), BF16),
            pltpu.VMEM((pd, 2 * nt, ns * rd, LANES), BF16),
            pltpu.VMEM((nz, pd, cg, GR, LANES), BF16),
            pltpu.VMEM((n, n, GR, LANES), F32),
            pltpu.VMEM((ns, occs, LANES), F32),
            pltpu.VMEM((nx, occs, LANES), F32),
            pltpu.VMEM((nz, mr, LANES), F32),
            pltpu.VMEM((ngp, GR, LANES), F32),
            pltpu.VMEM((ngp, GR, LANES), jnp.int16),
            pltpu.VMEM((ngp, 1, LANES), F32),
            pltpu.VMEM((nz, cg, GR, LANES), jnp.int16),
            pltpu.VMEM((nz, cg, 1, LANES), F32),
            pltpu.VMEM((2, LANES, LANES), F32),
            pltpu.VMEM((LANES, LANES), F32),
            pltpu.SemaphoreType.DMA,
            *sems,
        ],
        compiler_params=pltpu.CompilerParams(
            collective_id=0, has_side_effects=True, vmem_limit_bytes=48 * 1024 * 1024),
    )(amp, pair_list, tile_list, tile_table(tile_list, nt, ntv))
    virt = fin[:ng].astype(F32) * scale[:ng]
    return (virt.reshape(sd, rd, LANES), occ)


def solution(mesh):
    in_specs = (P(("groups", "pair"), "vir", "sub", None), P(("groups", "pair"), None), P())
    out_specs = (P(("groups", "vir"), "sub", None), P("groups", None))
    sizes = (mesh.shape["pair"], mesh.shape["vir"], mesh.shape["sub"])
    return jax.shard_map(functools.partial(shards, sizes), mesh=mesh, in_specs=in_specs,
                         out_specs=out_specs, check_vma=False)
```

```python
import functools
import math

import jax
import jax.numpy as jnp
from jax import lax
from jax.experimental import pallas as pl
from jax.experimental.pallas import tpu as pltpu
from jax.sharding import PartitionSpec as P

OCC = 256
GR = 16
LANES = 128
LEVELS = 32767.0
MESH = pl.DeviceIdType.MESH
F32 = jnp.float32
BF16 = jnp.bfloat16


def tile_table(tile_list, nt, ntv):
    grid = jnp.arange(ntv, dtype=jnp.int32)
    low = jnp.minimum(grid[:, None], grid[None, :])
    high = jnp.maximum(grid[:, None], grid[None, :])
    hit = (tile_list[:, 0][None, None] == low[:, :, None]) & (
        tile_list[:, 1][None, None] == high[:, :, None]
    )
    slots = jnp.arange(nt, dtype=jnp.int32)
    found = jnp.sum(jnp.where(hit, slots[None, None], 0), axis=2)
    return (found + jnp.where(grid[:, None] > grid[None, :], nt, 0)).reshape(-1)


def squeeze(vals):
    peak = jnp.maximum(jnp.max(jnp.abs(vals), axis=1, keepdims=True), 1e-33)
    whole = jnp.round(vals * (LEVELS / peak)).astype(jnp.int32)
    return whole.astype(jnp.int16), peak * (1.0 / LEVELS)


def widen(whole, scale):
    return whole.astype(jnp.int32).astype(F32) * scale


def kernel(dims, amp_in, pairs, tiles, table, fin, fin_scale, occ, amp, full, tile_buf, ga, acc,
           msg_s, msg_x, msg_z, part, part_q, part_scale, landed, landed_scale, orb_buf,
           couple_buf, in_sem, x_s, x_r, d_s, d_r, y_s, y_r, a_s, a_r, gs_s, gs_r, gx_s, gx_r, gz_s, gz_r,
           rs_s, rs_r, ag_s, ag_r, rt_s, rt_r, at_s, at_r):
    nz, nx, ns, pd, sd, gs, cg, nt, ntv, nch, waves = dims
    n = nz * pd
    occs = 2 * n
    rd = gs * GR
    tw = ns * rd
    z_at = lax.axis_index("pair")
    x_at = lax.axis_index("vir")
    s_at = lax.axis_index("sub")
    sizes = {"pair": nz, "vir": nx, "sub": ns}
    here = {"pair": z_at, "vir": x_at, "sub": s_at}

    def ahead(axis, by):
        return lax.rem(here[axis] + by, sizes[axis])

    def behind(axis, by):
        return lax.rem(here[axis] + sizes[axis] - by, sizes[axis])

    def send(src, dst, s_sem, r_sem, axis, by):
        return pltpu.make_async_remote_copy(
            src_ref=src, dst_ref=dst, send_sem=s_sem, recv_sem=r_sem,
            device_id={axis: ahead(axis, by)}, device_id_type=MESH)

    fetch = pltpu.make_async_copy(amp_in, amp, in_sem)
    fetch.start()
    barrier = pltpu.get_barrier_semaphore()
    count = 0
    for axis in ("sub", "vir", "pair"):
        for by in range(1, sizes[axis]):
            pl.semaphore_signal(barrier, inc=1, device_id={axis: ahead(axis, by)},
                                device_id_type=MESH)
            count += 1
    pl.semaphore_wait(barrier, count)
    fetch.wait()

    step = sd // nch * gs

    def x_copy(by, ch):
        rows = pl.ds(ch * step, step)
        return send(amp.at[:, rows], full.at[x_at, s_at, :, rows], x_s.at[by - 1, ch],
                    x_r.at[by - 1, ch], "vir", by)

    def relay(by, hop, ch):
        rows = pl.ds(ch * step, step)
        at = full.at[behind("vir", by), s_at, :, rows]
        return send(at, at, y_s.at[hop - 1, by - 1, ch], y_r.at[hop - 1, by - 1, ch], "sub", hop)

    def own_copy(hop):
        return send(amp, full.at[x_at, s_at], d_s.at[hop - 1], d_r.at[hop - 1], "sub", hop)

    def a2a_copy(by):
        rows = pl.ds(ahead("pair", by) * cg, cg)
        return send(amp.at[:, rows], ga.at[z_at], a_s.at[by - 1], a_r.at[by - 1], "pair", by)

    for ch in range(nch):
        for by in range(1, nx):
            x_copy(by, ch).start()
    for hop in range(1, ns):
        own_copy(hop).start()
    for by in range(1, nz):
        a2a_copy(by).start()

    full[x_at, s_at] = amp[...]
    ga[z_at] = amp[:, pl.ds(z_at * cg, cg)]
    lane_of = lax.broadcasted_iota(jnp.int32, (tw, LANES), 1)
    row_of = lax.broadcasted_iota(jnp.int32, (tw, LANES), 0)
    lower = lane_of <= row_of

    def build(x_from, lo, hi):
        def one(local, carry):
            slot = x_from * sd + local
            diagonal = tiles[slot, 0] == tiles[slot, 1]
            dropped = lower & diagonal
            groups = pl.ds(local * gs, gs)
            for k in range(pd):
                whole = jnp.concatenate(
                    [full[x_from, s, k, groups].reshape(rd, LANES) for s in range(ns)], axis=0)
                kept = jnp.where(dropped, 0.0, whole.astype(F32))
                turned = kept.T
                tile_buf[k, slot] = (kept - jnp.where(diagonal, turned, 0.0)).astype(BF16)
                tile_buf[k, nt + slot] = (-turned).astype(BF16)
            return carry

        lax.fori_loop(lo, hi, one, 0)

    for hop in range(1, ns):
        own_copy(hop).wait_recv()
    build(x_at, 0, sd)

    for by in range(1, nx):
        for ch in range(nch):
            x_copy(by, ch).wait_recv()
            for hop in range(1, ns):
                relay(by, hop, ch).start()
            for hop in range(1, ns):
                relay(by, hop, ch).wait_recv()
            build(behind("vir", by), ch * (sd // nch), (ch + 1) * (sd // nch))

    if part.shape[0] > sd * gs:
        spare = pl.ds(sd * gs, part.shape[0] - sd * gs)
        part[spare] = jnp.zeros((part.shape[0] - sd * gs, GR, LANES), F32)
        part_q[spare] = jnp.zeros((part.shape[0] - sd * gs, GR, LANES), jnp.int16)
        part_scale[spare] = jnp.zeros((part.shape[0] - sd * gs, 1, LANES), F32)

    def virt_slot(local, carry):
        slot = x_at * sd + local
        r = tiles[slot, 0]
        c = tiles[slot, 1]
        rows = pl.ds(pl.multiple_of(s_at * rd, rd), rd)
        total = None
        for k in range(pd):
            left = jnp.concatenate(
                [tile_buf[k, table[r * ntv + j], rows] for j in range(ntv)], axis=1)
            right = jnp.concatenate(
                [tile_buf[k, table[j * ntv + c]] for j in range(ntv)], axis=0)
            term = jnp.dot(left, right, preferred_element_type=F32)
            total = term if total is None else total + term
        groups = pl.ds(local * gs, gs)
        total = (-total).reshape(gs, GR, LANES)
        part[groups] = total
        part_q[groups], part_scale[groups] = squeeze(total)
        return carry

    half = cg // waves

    def rs_copies(to, source, wave):
        rows = pl.ds(to * cg + wave * half, half)
        return [
            pltpu.make_async_remote_copy(
                src_ref=src.at[rows], dst_ref=dst.at[source, pl.ds(wave * half, half)],
                send_sem=s_sem.at[to, wave], recv_sem=r_sem.at[source, wave], device_id={"pair": to}, device_id_type=MESH)
            for src, dst, s_sem, r_sem in ((part_q, landed, rs_s, rs_r),
                                           (part_scale, landed_scale, rt_s, rt_r))
        ]

    def ag_copies(by, wave):
        own = pl.ds(z_at * cg + wave * half, half)
        return [
            send(ref.at[own], ref.at[own], s_sem.at[by - 1, wave], r_sem.at[by - 1, wave],
                 "pair", by)
            for ref, s_sem, r_sem in ((fin, ag_s, ag_r), (fin_scale, at_s, at_r))
        ]

    done = 0
    for to in range(nz):
        until = min(sd, -(-cg * (to + 1) // gs))
        if until > done:
            lax.fori_loop(done, until, virt_slot, 0)
            done = until

        @pl.when(z_at != to)
        def _():
            for copy in rs_copies(to, z_at, 0):
                copy.start()

    for wave in range(1, waves):
        for by in range(1, nz):
            for copy in rs_copies(ahead("pair", by), z_at, wave):
                copy.start()

    for by in range(1, nz):
        a2a_copy(by).wait_recv()
    acc[...] = jnp.zeros_like(acc)
    g_lane = lax.broadcasted_iota(jnp.int32, (GR, LANES), 1)
    g_row = lax.broadcasted_iota(jnp.int32, (GR, LANES), 0)

    def gram_group(i, carry):
        at = z_at * cg + i
        slot = x_at * sd + jnp.minimum(at // gs, sd - 1)
        diagonal = tiles[slot, 0] == tiles[slot, 1]
        dropped = (g_lane <= g_row + (s_at * rd + lax.rem(at, gs) * GR)) & diagonal
        vals = ga[:, :, i].reshape(n, GR, LANES).astype(F32)
        vals = jnp.where(dropped[None], 0.0, vals)
        for p in range(n):
            acc[p] += vals * vals[p : p + 1]
        return carry

    lax.fori_loop(0, cg, gram_group, 0)
    m_lane = lax.broadcasted_iota(jnp.int32, (n, LANES), 1)
    grid = jnp.zeros((n, LANES), F32)
    for p in range(n):
        col = jnp.sum(jnp.sum(acc[p], axis=1), axis=1, keepdims=True)
        grid = jnp.where((m_lane == p) | (m_lane == p + n), col, grid)
    msg_s[0, 0:n] = grid
    msg_s[0, n:occs] = grid

    def gs_copy(hop):
        return send(msg_s.at[0], msg_s.at[hop], gs_s.at[hop - 1], gs_r.at[hop - 1], "sub", hop)

    def gx_copy(by):
        return send(msg_x.at[0], msg_x.at[by], gx_s.at[by - 1], gx_r.at[by - 1], "vir", by)

    def gz_copy(by):
        return send(msg_z.at[z_at], msg_z.at[z_at], gz_s.at[by - 1], gz_r.at[by - 1], "pair", by)

    for hop in range(1, ns):
        gs_copy(hop).start()

    for hop in range(1, ns):
        gs_copy(hop).wait_recv()
    msg_x[0] = sum((msg_s[hop] for hop in range(1, ns)), msg_s[0])
    for by in range(1, nx):
        gx_copy(by).start()
    total = msg_x[0]
    for by in range(1, nx):
        gx_copy(by).wait_recv()
        total = total + msg_x[by]
    msg_z[z_at, 0:occs] = total
    for k in range(pd):
        for e in range(2):
            msg_z[z_at, pl.ds(occs + 2 * k + e, 1)] = jnp.full((1, LANES), pairs[k, e], jnp.int32).astype(F32)
    for by in range(1, nz):
        gz_copy(by).start()

    for wave in range(waves):
        own = pl.ds(z_at * cg + wave * half, half)
        total = part[own]
        for by in range(1, nz):
            source = behind("pair", by)
            for copy in rs_copies(source, source, wave):
                copy.wait_recv()
            rows = pl.ds(wave * half, half)
            total = total + widen(landed[source, rows], landed_scale[source, rows])
        fin[own], fin_scale[own] = squeeze(total)
        for by in range(1, nz):
            for copy in ag_copies(by, wave):
                copy.start()

    for by in range(1, nz):
        gz_copy(by).wait_recv()
    gram = msg_z[0, 0:occs]
    for z in range(1, nz):
        gram = gram + msg_z[z, 0:occs]
    o_lane = lax.broadcasted_iota(jnp.int32, (1, LANES), 1)
    orb_lane = jnp.full((1, LANES), -1.0, F32)
    par_lane = jnp.full((1, LANES), -1.0, F32)
    orb_buf[...] = jnp.full(orb_buf.shape, -1.0, F32)
    for u in range(occs):
        p, e = u % n, u // n
        base = occs + 2 * (p % pd)
        orb = msg_z[p // pd, base + e : base + e + 1]
        par = msg_z[p // pd, base + 1 - e : base + 2 - e]
        orb_lane = jnp.where(o_lane == u, orb, orb_lane)
        par_lane = jnp.where(o_lane == u, par, par_lane)
        orb_buf[0, u : u + 1] = orb
        orb_buf[1, u : u + 1] = par
    c_lane = lax.broadcasted_iota(jnp.int32, (occs, LANES), 1)
    c_row = lax.broadcasted_iota(jnp.int32, (occs, LANES), 0)
    signed = jnp.where((c_lane < n) == (c_row < n), -gram, gram)
    couple_buf[...] = jnp.zeros_like(couple_buf)
    couple_buf[0:occs] = jnp.where(orb_buf[1, 0:occs] == par_lane, signed, 0.0)
    right_hot = (jnp.concatenate([orb_buf[0]] * (OCC // LANES), axis=1)
                 == lax.broadcasted_iota(jnp.int32, (LANES, OCC), 1).astype(F32)).astype(F32)
    left_hot = (lax.broadcasted_iota(jnp.int32, (OCC, LANES), 0).astype(F32)
                == orb_lane).astype(F32)
    inner = jnp.dot(couple_buf[...], right_hot, precision=lax.Precision.HIGHEST,
                    preferred_element_type=F32)
    occ[...] = jnp.dot(left_hot, inner, precision=lax.Precision.HIGHEST,
                       preferred_element_type=F32)

    for by in range(1, nz):
        for wave in range(waves):
            for copy in ag_copies(by, wave):
                copy.wait_recv()

    for by in range(1, nx):
        gx_copy(by).wait_send()
        for ch in range(nch):
            x_copy(by, ch).wait_send()
            for hop in range(1, ns):
                relay(by, hop, ch).wait_send()
    for hop in range(1, ns):
        own_copy(hop).wait_send()
        gs_copy(hop).wait_send()
    for by in range(1, nz):
        a2a_copy(by).wait_send()
        gz_copy(by).wait_send()
        for wave in range(waves):
            for copy in ag_copies(by, wave) + rs_copies(ahead("pair", by), z_at, wave):
                copy.wait_send()


def shards(sizes, amplitudes, pair_list, tile_list):
    nz, nx, ns = sizes
    pd, sd, rd, _ = amplitudes.shape
    nt = tile_list.shape[0]
    ntv = (math.isqrt(8 * nt + 1) - 1) // 2
    gs = rd // GR
    ng = sd * gs
    cg = -(-ng // nz)
    ngp = cg * nz
    nch = 6 if sd % 6 == 0 else 3 if sd % 3 == 0 else 1
    n = nz * pd
    occs = 2 * n
    amp = amplitudes.reshape(pd, ng, GR, LANES)
    if ngp > ng:
        amp = jnp.pad(amp, ((0, 0), (0, ngp - ng), (0, 0), (0, 0)))
    mr = -(-(occs + 2 * pd) // 8) * 8
    waves = 2 if cg % 2 == 0 else 1
    dims = (nz, nx, ns, pd, sd, gs, cg, nt, ntv, nch, waves)
    vmem = pl.BlockSpec(memory_space=pltpu.VMEM)
    smem = pl.BlockSpec(memory_space=pltpu.SMEM)

    def dma(*shape):
        return pltpu.SemaphoreType.DMA(tuple(max(1, d) for d in shape))

    sems = []
    for shape in ((nx - 1, nch), (ns - 1,), (ns - 1, nx - 1, nch), (nz - 1,), (ns - 1,),
                  (nx - 1,), (nz - 1,), (nz, waves), (nz - 1, waves), (nz, waves),
                  (nz - 1, waves)):
        sems += [dma(*shape), dma(*shape)]
    fin, scale, occ = pl.pallas_call(
        functools.partial(kernel, dims),
        out_shape=(jax.ShapeDtypeStruct((ngp, GR, LANES), jnp.int16),
                   jax.ShapeDtypeStruct((ngp, 1, LANES), F32),
                   jax.ShapeDtypeStruct((OCC, OCC), F32)),
        in_specs=[pl.BlockSpec(memory_space=pltpu.MemorySpace.HBM), smem, smem, smem],
        out_specs=(vmem, vmem, vmem),
        scratch_shapes=[
            pltpu.VMEM((pd, ngp, GR, LANES), BF16),
            pltpu.VMEM((nx, ns, pd, ngp, GR, LANES), BF16),
            pltpu.VMEM((pd, 2 * nt, ns * rd, LANES), BF16),
            pltpu.VMEM((nz, pd, cg, GR, LANES), BF16),
            pltpu.VMEM((n, n, GR, LANES), F32),
            pltpu.VMEM((ns, occs, LANES), F32),
            pltpu.VMEM((nx, occs, LANES), F32),
            pltpu.VMEM((nz, mr, LANES), F32),
            pltpu.VMEM((ngp, GR, LANES), F32),
            pltpu.VMEM((ngp, GR, LANES), jnp.int16),
            pltpu.VMEM((ngp, 1, LANES), F32),
            pltpu.VMEM((nz, cg, GR, LANES), jnp.int16),
            pltpu.VMEM((nz, cg, 1, LANES), F32),
            pltpu.VMEM((2, LANES, LANES), F32),
            pltpu.VMEM((LANES, LANES), F32),
            pltpu.SemaphoreType.DMA,
            *sems,
        ],
        compiler_params=pltpu.CompilerParams(
            collective_id=0, has_side_effects=True, vmem_limit_bytes=48 * 1024 * 1024),
    )(amp, pair_list, tile_list, tile_table(tile_list, nt, ntv))
    virt = fin[:ng].astype(F32) * scale[:ng]
    return (virt.reshape(sd, rd, LANES), occ)


def solution(mesh):
    in_specs = (P(("groups", "pair"), "vir", "sub", None), P(("groups", "pair"), None), P())
    out_specs = (P(("groups", "vir"), "sub", None), P("groups", None))
    sizes = (mesh.shape["pair"], mesh.shape["vir"], mesh.shape["sub"])
    return jax.shard_map(functools.partial(shards, sizes), mesh=mesh, in_specs=in_specs,
                         out_specs=out_specs, check_vma=False)
```

```python
import functools
import math

import jax
import jax.numpy as jnp
from jax import lax
from jax.experimental import pallas as pl
from jax.experimental.pallas import tpu as pltpu
from jax.sharding import PartitionSpec as P

OCC = 256
GR = 16
LANES = 128
LEVELS = 32767.0
MESH = pl.DeviceIdType.MESH
F32 = jnp.float32
BF16 = jnp.bfloat16


def tile_table(tile_list, nt, ntv):
    grid = jnp.arange(ntv, dtype=jnp.int32)
    low = jnp.minimum(grid[:, None], grid[None, :])
    high = jnp.maximum(grid[:, None], grid[None, :])
    hit = (tile_list[:, 0][None, None] == low[:, :, None]) & (
        tile_list[:, 1][None, None] == high[:, :, None]
    )
    slots = jnp.arange(nt, dtype=jnp.int32)
    found = jnp.sum(jnp.where(hit, slots[None, None], 0), axis=2)
    return (found + jnp.where(grid[:, None] > grid[None, :], nt, 0)).reshape(-1)


def squeeze(vals):
    peak = jnp.maximum(jnp.max(jnp.abs(vals), axis=1, keepdims=True), 1e-33)
    whole = jnp.round(vals * (LEVELS / peak)).astype(jnp.int32)
    return whole.astype(jnp.int16), peak * (1.0 / LEVELS)


def widen(whole, scale):
    return whole.astype(jnp.int32).astype(F32) * scale


def kernel(dims, amp_in, pairs, tiles, table, fin, fin_scale, occ, amp, full, tile_buf, ga, acc,
           msg_s, msg_x, msg_z, part, part_q, part_scale, landed, landed_scale, orb_buf,
           couple_buf, in_sem, x_s, x_r, d_s, d_r, y_s, y_r, a_s, a_r, gs_s, gs_r, gx_s, gx_r, gz_s, gz_r,
           rs_s, rs_r, ag_s, ag_r, rt_s, rt_r, at_s, at_r):
    nz, nx, ns, pd, sd, gs, cg, nt, ntv, nch, waves = dims
    n = nz * pd
    occs = 2 * n
    rd = gs * GR
    tw = ns * rd
    z_at = lax.axis_index("pair")
    x_at = lax.axis_index("vir")
    s_at = lax.axis_index("sub")
    sizes = {"pair": nz, "vir": nx, "sub": ns}
    here = {"pair": z_at, "vir": x_at, "sub": s_at}

    def ahead(axis, by):
        return lax.rem(here[axis] + by, sizes[axis])

    def behind(axis, by):
        return lax.rem(here[axis] + sizes[axis] - by, sizes[axis])

    def send(src, dst, s_sem, r_sem, axis, by):
        return pltpu.make_async_remote_copy(
            src_ref=src, dst_ref=dst, send_sem=s_sem, recv_sem=r_sem,
            device_id={axis: ahead(axis, by)}, device_id_type=MESH)

    fetch = pltpu.make_async_copy(amp_in, amp, in_sem)
    fetch.start()
    barrier = pltpu.get_barrier_semaphore()
    count = 0
    for axis in ("sub", "vir", "pair"):
        for by in range(1, sizes[axis]):
            pl.semaphore_signal(barrier, inc=1, device_id={axis: ahead(axis, by)},
                                device_id_type=MESH)
            count += 1
    pl.semaphore_wait(barrier, count)
    fetch.wait()

    step = sd // nch * gs

    def x_copy(by, ch):
        rows = pl.ds(ch * step, step)
        return send(amp.at[:, rows], full.at[x_at, s_at, :, rows], x_s.at[by - 1, ch],
                    x_r.at[by - 1, ch], "vir", by)

    def relay(by, hop, ch):
        rows = pl.ds(ch * step, step)
        at = full.at[behind("vir", by), s_at, :, rows]
        return send(at, at, y_s.at[hop - 1, by - 1, ch], y_r.at[hop - 1, by - 1, ch], "sub", hop)

    def own_copy(hop):
        return send(amp, full.at[x_at, s_at], d_s.at[hop - 1], d_r.at[hop - 1], "sub", hop)

    def a2a_copy(by):
        rows = pl.ds(ahead("pair", by) * cg, cg)
        return send(amp.at[:, rows], ga.at[z_at], a_s.at[by - 1], a_r.at[by - 1], "pair", by)

    for ch in range(nch):
        for by in range(1, nx):
            x_copy(by, ch).start()
    for hop in range(1, ns):
        own_copy(hop).start()
    for by in range(1, nz):
        a2a_copy(by).start()

    full[x_at, s_at] = amp[...]
    ga[z_at] = amp[:, pl.ds(z_at * cg, cg)]
    lane_of = lax.broadcasted_iota(jnp.int32, (tw, LANES), 1)
    row_of = lax.broadcasted_iota(jnp.int32, (tw, LANES), 0)
    lower = lane_of <= row_of

    def build(x_from, lo, hi):
        def one(local, carry):
            slot = x_from * sd + local
            diagonal = tiles[slot, 0] == tiles[slot, 1]
            dropped = lower & diagonal
            groups = pl.ds(local * gs, gs)
            for k in range(pd):
                whole = jnp.concatenate(
                    [full[x_from, s, k, groups].reshape(rd, LANES) for s in range(ns)], axis=0)
                kept = jnp.where(dropped, 0.0, whole.astype(F32))
                turned = kept.T
                tile_buf[k, slot] = (kept - jnp.where(diagonal, turned, 0.0)).astype(BF16)
                tile_buf[k, nt + slot] = (-turned).astype(BF16)
            return carry

        lax.fori_loop(lo, hi, one, 0)

    for hop in range(1, ns):
        own_copy(hop).wait_recv()
    build(x_at, 0, sd)

    for by in range(1, nx):
        for ch in range(nch):
            x_copy(by, ch).wait_recv()
            for hop in range(1, ns):
                relay(by, hop, ch).start()
            for hop in range(1, ns):
                relay(by, hop, ch).wait_recv()
            build(behind("vir", by), ch * (sd // nch), (ch + 1) * (sd // nch))

    if part.shape[0] > sd * gs:
        spare = pl.ds(sd * gs, part.shape[0] - sd * gs)
        part[spare] = jnp.zeros((part.shape[0] - sd * gs, GR, LANES), F32)
        part_q[spare] = jnp.zeros((part.shape[0] - sd * gs, GR, LANES), jnp.int16)
        part_scale[spare] = jnp.zeros((part.shape[0] - sd * gs, 1, LANES), F32)

    def virt_slot(local, carry):
        slot = x_at * sd + local
        r = tiles[slot, 0]
        c = tiles[slot, 1]
        rows = pl.ds(pl.multiple_of(s_at * rd, rd), rd)
        total = None
        for k in range(pd):
            left = jnp.concatenate(
                [tile_buf[k, table[r * ntv + j], rows] for j in range(ntv)], axis=1)
            right = jnp.concatenate(
                [tile_buf[k, table[j * ntv + c]] for j in range(ntv)], axis=0)
            term = jnp.dot(left, right, preferred_element_type=F32)
            total = term if total is None else total + term
        groups = pl.ds(local * gs, gs)
        total = (-total).reshape(gs, GR, LANES)
        part[groups] = total
        part_q[groups], part_scale[groups] = squeeze(total)
        return carry

    half = cg // waves

    def rs_copies(to, source, wave):
        rows = pl.ds(to * cg + wave * half, half)
        return [
            pltpu.make_async_remote_copy(
                src_ref=src.at[rows], dst_ref=dst.at[source, pl.ds(wave * half, half)],
                send_sem=s_sem.at[to, wave], recv_sem=r_sem.at[source, wave], device_id={"pair": to}, device_id_type=MESH)
            for src, dst, s_sem, r_sem in ((part_q, landed, rs_s, rs_r),
                                           (part_scale, landed_scale, rt_s, rt_r))
        ]

    def ag_copies(by, wave):
        own = pl.ds(z_at * cg + wave * half, half)
        return [
            send(ref.at[own], ref.at[own], s_sem.at[by - 1, wave], r_sem.at[by - 1, wave],
                 "pair", by)
            for ref, s_sem, r_sem in ((fin, ag_s, ag_r), (fin_scale, at_s, at_r))
        ]

    done = 0
    for to in range(nz):
        until = min(sd, -(-cg * (to + 1) // gs))
        if until > done:
            lax.fori_loop(done, until, virt_slot, 0)
            done = until

        @pl.when(z_at != to)
        def _():
            for copy in rs_copies(to, z_at, 0):
                copy.start()

    for wave in range(1, waves):
        for by in range(1, nz):
            for copy in rs_copies(ahead("pair", by), z_at, wave):
                copy.start()

    for by in range(1, nz):
        a2a_copy(by).wait_recv()
    acc[...] = jnp.zeros_like(acc)
    g_lane = lax.broadcasted_iota(jnp.int32, (GR, LANES), 1)
    g_row = lax.broadcasted_iota(jnp.int32, (GR, LANES), 0)

    def gram_group(i, carry):
        at = z_at * cg + i
        slot = x_at * sd + jnp.minimum(at // gs, sd - 1)
        diagonal = tiles[slot, 0] == tiles[slot, 1]
        dropped = (g_lane <= g_row + (s_at * rd + lax.rem(at, gs) * GR)) & diagonal
        vals = ga[:, :, i].reshape(n, GR, LANES).astype(F32)
        vals = jnp.where(dropped[None], 0.0, vals)
        for p in range(n):
            acc[p] += vals * vals[p : p + 1]
        return carry

    lax.fori_loop(0, cg, gram_group, 0)
    m_lane = lax.broadcasted_iota(jnp.int32, (n, LANES), 1)
    grid = jnp.zeros((n, LANES), F32)
    for p in range(n):
        col = jnp.sum(jnp.sum(acc[p], axis=1), axis=1, keepdims=True)
        grid = jnp.where((m_lane == p) | (m_lane == p + n), col, grid)
    msg_s[0, 0:n] = grid
    msg_s[0, n:occs] = grid

    def gs_copy(hop):
        return send(msg_s.at[0], msg_s.at[hop], gs_s.at[hop - 1], gs_r.at[hop - 1], "sub", hop)

    def gx_copy(by):
        return send(msg_x.at[0], msg_x.at[by], gx_s.at[by - 1], gx_r.at[by - 1], "vir", by)

    def gz_copy(by):
        return send(msg_z.at[z_at], msg_z.at[z_at], gz_s.at[by - 1], gz_r.at[by - 1], "pair", by)

    for hop in range(1, ns):
        gs_copy(hop).start()

    for hop in range(1, ns):
        gs_copy(hop).wait_recv()
    msg_x[0] = sum((msg_s[hop] for hop in range(1, ns)), msg_s[0])
    for by in range(1, nx):
        gx_copy(by).start()
    for wave in range(waves):
        own = pl.ds(z_at * cg + wave * half, half)
        total = part[own]
        for by in range(1, nz):
            source = behind("pair", by)
            for copy in rs_copies(source, source, wave):
                copy.wait_recv()
            rows = pl.ds(wave * half, half)
            total = total + widen(landed[source, rows], landed_scale[source, rows])
        fin[own], fin_scale[own] = squeeze(total)
        for by in range(1, nz):
            for copy in ag_copies(by, wave):
                copy.start()
        if wave == 0:
            joined = msg_x[0]
            for by in range(1, nx):
                gx_copy(by).wait_recv()
                joined = joined + msg_x[by]
            msg_z[z_at, 0:occs] = joined
            for k in range(pd):
                for e in range(2):
                    msg_z[z_at, pl.ds(occs + 2 * k + e, 1)] = jnp.full((1, LANES), pairs[k, e], jnp.int32).astype(F32)
            for by in range(1, nz):
                gz_copy(by).start()

    for by in range(1, nz):
        gz_copy(by).wait_recv()
    gram = msg_z[0, 0:occs]
    for z in range(1, nz):
        gram = gram + msg_z[z, 0:occs]
    o_lane = lax.broadcasted_iota(jnp.int32, (1, LANES), 1)
    orb_lane = jnp.full((1, LANES), -1.0, F32)
    par_lane = jnp.full((1, LANES), -1.0, F32)
    orb_buf[...] = jnp.full(orb_buf.shape, -1.0, F32)
    for u in range(occs):
        p, e = u % n, u // n
        base = occs + 2 * (p % pd)
        orb = msg_z[p // pd, base + e : base + e + 1]
        par = msg_z[p // pd, base + 1 - e : base + 2 - e]
        orb_lane = jnp.where(o_lane == u, orb, orb_lane)
        par_lane = jnp.where(o_lane == u, par, par_lane)
        orb_buf[0, u : u + 1] = orb
        orb_buf[1, u : u + 1] = par
    c_lane = lax.broadcasted_iota(jnp.int32, (occs, LANES), 1)
    c_row = lax.broadcasted_iota(jnp.int32, (occs, LANES), 0)
    signed = jnp.where((c_lane < n) == (c_row < n), -gram, gram)
    couple_buf[...] = jnp.zeros_like(couple_buf)
    couple_buf[0:occs] = jnp.where(orb_buf[1, 0:occs] == par_lane, signed, 0.0)
    right_hot = (jnp.concatenate([orb_buf[0]] * (OCC // LANES), axis=1)
                 == lax.broadcasted_iota(jnp.int32, (LANES, OCC), 1).astype(F32)).astype(F32)
    left_hot = (lax.broadcasted_iota(jnp.int32, (OCC, LANES), 0).astype(F32)
                == orb_lane).astype(F32)
    inner = jnp.dot(couple_buf[...], right_hot, precision=lax.Precision.HIGHEST,
                    preferred_element_type=F32)
    occ[...] = jnp.dot(left_hot, inner, precision=lax.Precision.HIGHEST,
                       preferred_element_type=F32)

    for by in range(1, nz):
        for wave in range(waves):
            for copy in ag_copies(by, wave):
                copy.wait_recv()

    for by in range(1, nx):
        gx_copy(by).wait_send()
        for ch in range(nch):
            x_copy(by, ch).wait_send()
            for hop in range(1, ns):
                relay(by, hop, ch).wait_send()
    for hop in range(1, ns):
        own_copy(hop).wait_send()
        gs_copy(hop).wait_send()
    for by in range(1, nz):
        a2a_copy(by).wait_send()
        gz_copy(by).wait_send()
        for wave in range(waves):
            for copy in ag_copies(by, wave) + rs_copies(ahead("pair", by), z_at, wave):
                copy.wait_send()


def shards(sizes, amplitudes, pair_list, tile_list):
    nz, nx, ns = sizes
    pd, sd, rd, _ = amplitudes.shape
    nt = tile_list.shape[0]
    ntv = (math.isqrt(8 * nt + 1) - 1) // 2
    gs = rd // GR
    ng = sd * gs
    cg = -(-ng // nz)
    ngp = cg * nz
    nch = 6 if sd % 6 == 0 else 3 if sd % 3 == 0 else 1
    n = nz * pd
    occs = 2 * n
    amp = amplitudes.reshape(pd, ng, GR, LANES)
    if ngp > ng:
        amp = jnp.pad(amp, ((0, 0), (0, ngp - ng), (0, 0), (0, 0)))
    mr = -(-(occs + 2 * pd) // 8) * 8
    waves = 2 if cg % 2 == 0 else 1
    dims = (nz, nx, ns, pd, sd, gs, cg, nt, ntv, nch, waves)
    vmem = pl.BlockSpec(memory_space=pltpu.VMEM)
    smem = pl.BlockSpec(memory_space=pltpu.SMEM)

    def dma(*shape):
        return pltpu.SemaphoreType.DMA(tuple(max(1, d) for d in shape))

    sems = []
    for shape in ((nx - 1, nch), (ns - 1,), (ns - 1, nx - 1, nch), (nz - 1,), (ns - 1,),
                  (nx - 1,), (nz - 1,), (nz, waves), (nz - 1, waves), (nz, waves),
                  (nz - 1, waves)):
        sems += [dma(*shape), dma(*shape)]
    fin, scale, occ = pl.pallas_call(
        functools.partial(kernel, dims),
        out_shape=(jax.ShapeDtypeStruct((ngp, GR, LANES), jnp.int16),
                   jax.ShapeDtypeStruct((ngp, 1, LANES), F32),
                   jax.ShapeDtypeStruct((OCC, OCC), F32)),
        in_specs=[pl.BlockSpec(memory_space=pltpu.MemorySpace.HBM), smem, smem, smem],
        out_specs=(vmem, vmem, vmem),
        scratch_shapes=[
            pltpu.VMEM((pd, ngp, GR, LANES), BF16),
            pltpu.VMEM((nx, ns, pd, ngp, GR, LANES), BF16),
            pltpu.VMEM((pd, 2 * nt, ns * rd, LANES), BF16),
            pltpu.VMEM((nz, pd, cg, GR, LANES), BF16),
            pltpu.VMEM((n, n, GR, LANES), F32),
            pltpu.VMEM((ns, occs, LANES), F32),
            pltpu.VMEM((nx, occs, LANES), F32),
            pltpu.VMEM((nz, mr, LANES), F32),
            pltpu.VMEM((ngp, GR, LANES), F32),
            pltpu.VMEM((ngp, GR, LANES), jnp.int16),
            pltpu.VMEM((ngp, 1, LANES), F32),
            pltpu.VMEM((nz, cg, GR, LANES), jnp.int16),
            pltpu.VMEM((nz, cg, 1, LANES), F32),
            pltpu.VMEM((2, LANES, LANES), F32),
            pltpu.VMEM((LANES, LANES), F32),
            pltpu.SemaphoreType.DMA,
            *sems,
        ],
        compiler_params=pltpu.CompilerParams(
            collective_id=0, has_side_effects=True, vmem_limit_bytes=48 * 1024 * 1024),
    )(amp, pair_list, tile_list, tile_table(tile_list, nt, ntv))
    virt = fin[:ng].astype(F32) * scale[:ng]
    return (virt.reshape(sd, rd, LANES), occ)


def solution(mesh):
    in_specs = (P(("groups", "pair"), "vir", "sub", None), P(("groups", "pair"), None), P())
    out_specs = (P(("groups", "vir"), "sub", None), P("groups", None))
    sizes = (mesh.shape["pair"], mesh.shape["vir"], mesh.shape["sub"])
    return jax.shard_map(functools.partial(shards, sizes), mesh=mesh, in_specs=in_specs,
                         out_specs=out_specs, check_vma=False)
```
